32 devices in a mesh: dp: 4 (over x, core), expert: 8 (over z, y).
Axes of the slice: x: 2, y: 2, z: 4, core: 2. Of those that a mesh axis runs over, the one named last changes fastest.
Arguments:
- tokens: bfloat16 [4096, 1024], P(('dp', 'expert')), may hold values from -6 to 6
- task_ids: int32 [32], P('dp'), may hold values from 0 to 5
- routing: int32 [32, 2], P('dp'), may hold values from 0 to 7, all different within a row; in each aligned block of 8 rows (0 to 7, 8 to 15, ...) at most 3 rows name the same one
- gate_weight: bfloat16 [1024, 48], replicated, may hold values from -0.1875 to 0.1875
- w_in: bfloat16 [8, 1024, 4096], P('expert', None, 'dp'), may hold values from -0.1875 to 0.1875
- w_out: bfloat16 [8, 4096, 1024], P('expert', 'dp'), may hold values from -0.09375 to 0.09375
Outputs:
- mixed: bfloat16 [4096, 1024], P(('dp', 'expert'))
The draws below stay inside these ranges and needn't reach their ends.
Inputs may be any that keep to these rules, and one draw needn't show every extreme that they name: `routing`: each row names two different experts. Within the 8 blocks of one index of dp no expert is named more than 3 times, a bound that some block reaches.
All inputs are finite; a program needn't handle non-finite values.
Results may differ from the reference program's by a relative error of at most 0.015.
Values may be sent and summed in bfloat16 or wider, within the bound.
A program may use at most 64 MiB of HBM per device.

```python
import math
import jax
import jax.numpy as jnp
import numpy as np
from jax import lax

D = 1024
FF = 4096
TASKS = 6
BLK = 128
EXPERTS = 8
ROWBLK = 8
CAP = 3
BLOCKS = 32
TOKENS = 4096
N_DP = 4


def with_ends(array, stream_key, smallest, high):
    extent = array.shape
    index_at = [jax.random.randint(jax.random.fold_in(stream_key, axis), (), 0, extent[axis]) for axis in range(len(extent))]
    array = array.at[tuple(index_at)].set(smallest)
    longest = extent.index(max(extent))
    index_at[longest] = (index_at[longest] + 1) % extent[longest]
    return array.at[tuple(index_at)].set(high)


def level_of(stream_key, shape, shards, smallest, largest):
    def one(dim, blocks):
        draws = jax.random.uniform(jax.random.fold_in(jax.random.fold_in(stream_key, 6), dim), (blocks,), jnp.float32, smallest / len(shards), largest / len(shards))
        return jnp.repeat(jnp.exp(draws), shape[dim] // blocks).reshape((-1,) + (1,) * (len(shape) - dim - 1))

    loudness = one(*shards[0])
    for cut in shards[1:]:
        loudness = loudness * one(*cut)
    return loudness


def routed_block(key, own, number, rows, count, top, most, lean):
    sequence = jax.random.permutation(key, count)
    heavy_load, ordinary = load_shares(count, rows * top, most, lean, True), load_shares(count, rows * top, most, lean, False)
    places = jnp.arange(count)

    def named(tallies, offset_by):
        used = int((tallies > 0).sum())
        fixed = max(1, used // 4)
        shifted = fixed + (places - fixed + offset_by * (used - fixed)) % max(1, count - fixed)
        return jnp.zeros((count,), jnp.int32).at[sequence[jnp.where(places < fixed, places, shifted)]].set(jnp.asarray(tallies, jnp.int32))

    tallies = jnp.where(number % 4 == 0, named(heavy_load, number // 4), named(ordinary, number - number // 4 - 1))
    mixed = jax.random.permutation(jax.random.fold_in(own, 3), count)
    source_of, taker = mixed[0:count // 2 * 2:2], mixed[1:count // 2 * 2:2]
    slack = jnp.minimum(tallies[source_of] - 1, most - tallies[taker]) // 2
    slack = jnp.where((source_of == sequence[0]) | (taker == sequence[0]) | (tallies[taker] == 0), 0, jnp.maximum(slack, 0))
    shifted = jax.random.randint(jax.random.fold_in(own, 4), (count // 2,), 0, 1 << 20) % (slack + 1)
    tallies = tallies.at[source_of].add(-shifted).at[taker].add(shifted)
    members = jnp.searchsorted(jnp.cumsum(tallies), jnp.arange(rows * top), side="right").astype(jnp.int32)
    table = members.reshape(top, rows).T
    table = table[jax.random.permutation(jax.random.fold_in(own, 1), rows)]
    offset_by = jax.random.randint(jax.random.fold_in(own, 2), (rows, 1), 0, top)
    return jnp.take_along_axis(table, (jnp.arange(top)[None, :] + offset_by) % top, axis=1)


def load_shares(count, total, bound, slope, full):
    weights = [(1 << 20) // math.isqrt(grade ** slope) + 1 for grade in range(1, count + 1)]
    largest = bound if full else min(bound, max(-(-total // count), total * weights[0] // sum(weights)))
    least = 1 if total - largest >= count - 1 else 0
    given, surplus = [largest] + [least] * (count - 1), total - largest - least * (count - 1)
    while surplus > 0:
        candidates = [i for i in range(1, count) if given[i] < largest] or [i for i in range(1, count) if given[i] < bound]
        mass, left = sum([weights[i] for i in candidates]), surplus
        for i in candidates:
            addition = min(bound - given[i], max(1, left * weights[i] // mass), surplus)
            given[i] = given[i] + addition
            surplus = surplus - addition
    return np.array(given)


def bell_draw(stream_key, dims, width, most, shards=(), dtype=jnp.bfloat16):
    level = level_of(stream_key, dims, shards, -0.22, 0.18) if shards else 1.0
    entries = jax.random.normal(stream_key, dims, jnp.float32) * width * level
    return jnp.minimum(jnp.maximum(entries, -most), most).astype(dtype)


def setup_inputs(seed: int = 0) -> dict:
    splits = jax.random.split(jax.random.key(seed), 7)
    tokens = bell_draw(splits[0], (TOKENS, D), 1.0, 6.0, ((0, 32),))
    task_ids = with_ends(jax.random.randint(splits[1], (BLOCKS,), 0, TASKS), jax.random.fold_in(splits[1], 1), 0, TASKS - 1).astype(jnp.int32)
    routing_keys = jax.random.split(jax.random.fold_in(splits[2], 1), BLOCKS // ROWBLK)
    routing_turns = jax.random.permutation(jax.random.fold_in(splits[2], 3), BLOCKS // ROWBLK)
    routing = jax.vmap(lambda own, number: routed_block(jax.random.fold_in(splits[2], 2), own, number, ROWBLK, EXPERTS, 2, CAP, 2))(routing_keys, routing_turns).reshape((BLOCKS, 2))
    gate_weight = bell_draw(splits[3], (D, TASKS * EXPERTS), D ** -0.5, 0.1875)
    w_in = bell_draw(splits[4], (EXPERTS, D, FF), D ** -0.5, 0.1875, ((0, 8), (2, 4)))
    w_out = bell_draw(splits[5], (EXPERTS, FF, D), FF ** -0.5, 0.09375, ((0, 8), (1, 4)))
    return dict(tokens=tokens, task_ids=task_ids, routing=routing, gate_weight=gate_weight, w_in=w_in, w_out=w_out)


def expert_output(block_rows, expert_id, w_in, w_out):
    hidden = jax.nn.gelu(jnp.dot(block_rows, w_in[expert_id], preferred_element_type=jnp.float32)).astype(jnp.bfloat16)
    slice_width = FF // N_DP
    hidden_split = hidden.reshape(BLK, N_DP, slice_width).astype(jnp.float32)
    weight_split = w_out[expert_id].reshape(N_DP, slice_width, D).astype(jnp.float32)
    partials = jnp.einsum("bjs,jsd->jbd", hidden_split, weight_split).astype(jnp.bfloat16)
    partials = lax.optimization_barrier(partials).astype(jnp.float32)
    return jnp.sum(partials, axis=0)


def reference(tokens, task_ids, routing, gate_weight, w_in, w_out):
    token_blocks = tokens.reshape(BLOCKS, BLK, D)

    def per_block(inputs):
        block_rows, task_id, route_pair = inputs
        logits = jnp.dot(block_rows, gate_weight, preferred_element_type=jnp.float32).reshape(BLK, TASKS, EXPERTS)
        task_logits = lax.dynamic_index_in_dim(logits, task_id, 1, keepdims=False)
        logit_first = task_logits[:, route_pair[0]]
        logit_second = task_logits[:, route_pair[1]]
        gate_first = jax.nn.sigmoid(logit_first - logit_second)
        gate_second = jax.nn.sigmoid(logit_second - logit_first)
        first_sum = expert_output(block_rows, route_pair[0], w_in, w_out)
        second_sum = expert_output(block_rows, route_pair[1], w_in, w_out)
        gated_first = (gate_first[:, None] * first_sum).astype(jnp.bfloat16)
        gated_second = (gate_second[:, None] * second_sum).astype(jnp.bfloat16)
        return (gated_first.astype(jnp.float32) + gated_second.astype(jnp.float32)).astype(jnp.bfloat16)

    mixed = lax.map(per_block, (token_blocks, task_ids, routing))
    return mixed.reshape(TOKENS, D)
```

```python
import jax
import jax.numpy as jnp
from jax import lax
from jax.sharding import PartitionSpec as P

BLK = 128


def shards(tokens, task_ids, routing, gate_weight, w_in, w_out):
    n_experts = lax.axis_size("expert")
    n_dp = lax.axis_size("dp")
    my_expert = lax.axis_index("expert")
    local_rows, width_model = tokens.shape
    block_total = routing.shape[0]
    block_here = local_rows // BLK
    capacity = 2 * block_here + 1
    chosen = routing == my_expert
    taken_flag = jnp.any(chosen, axis=1).astype(jnp.int32)
    ranked = jnp.cumsum(taken_flag) - taken_flag
    slot_ids = jnp.arange(capacity, dtype=jnp.int32)
    select_mask = (taken_flag[None, :] == 1) & (ranked[None, :] == slot_ids[:, None])
    select_float = select_mask.astype(jnp.bfloat16)
    select_int = select_mask.astype(jnp.int32)
    other_id = jnp.where(chosen[:, 0], routing[:, 1], routing[:, 0])
    slot_task = jnp.sum(select_int * task_ids[None, :], axis=1)
    slot_other = jnp.sum(select_int * other_id[None, :], axis=1)
    slot_valid = jnp.sum(select_int, axis=1).astype(jnp.float32)
    slot_block = jnp.sum(
        select_int * jnp.arange(block_total, dtype=jnp.int32)[None, :], axis=1
    )
    row_tokens = lax.all_gather(tokens, "expert", axis=0, tiled=True)
    picked = jnp.concatenate(
        [
            lax.dynamic_slice_in_dim(row_tokens, slot_block[slot] * BLK, BLK, 0)
            for slot in range(capacity)
        ],
        axis=0,
    )
    column_slots = lax.all_gather(picked, "dp", axis=0, tiled=True)
    hidden = jax.nn.gelu(
        jnp.dot(column_slots, w_in[0], preferred_element_type=jnp.float32)
    ).astype(jnp.bfloat16)
    partial = jnp.dot(hidden, w_out[0], preferred_element_type=jnp.float32).astype(jnp.bfloat16)
    running = lax.psum_scatter(partial, "dp", scatter_dimension=0, tiled=True)

    gate_columns = gate_weight.shape[1]
    logits = jnp.dot(picked, gate_weight, preferred_element_type=jnp.float32).reshape(
        capacity, BLK, gate_columns
    )
    column_ids = jnp.arange(gate_columns, dtype=jnp.int32)
    sign = (column_ids[None, :] == (slot_task * n_experts + my_expert)[:, None]).astype(
        jnp.float32
    ) - (column_ids[None, :] == (slot_task * n_experts + slot_other)[:, None]).astype(jnp.float32)
    weights = (
        jax.nn.sigmoid(jnp.sum(logits * sign[:, None, :], axis=2)) * slot_valid[:, None]
    ).reshape(capacity * BLK)
    gated = (weights[:, None] * running.astype(jnp.float32)).astype(jnp.bfloat16)
    gated = gated.reshape(capacity, BLK, width_model)
    placed = jnp.zeros((block_total, BLK, width_model), jnp.bfloat16)
    for slot in range(capacity):
        placed = jnp.where(select_mask[slot][:, None, None], gated[slot][None], placed)
    return lax.psum_scatter(
        placed.reshape(block_total * BLK, width_model), "expert", scatter_dimension=0, tiled=True
    )


def solution(mesh):
    placed = (
        P(("dp", "expert"), None),
        P("dp"),
        P("dp", None),
        P(),
        P("expert", None, "dp"),
        P("expert", "dp", None),
    )
    return jax.shard_map(
        shards, mesh=mesh, in_specs=placed, out_specs=P(("dp", "expert"), None), check_vma=False
    )
```

```python
import functools

import jax
import jax.numpy as jnp
from jax import lax
from jax.experimental import pallas as pl
from jax.experimental.pallas import tpu as pltpu
from jax.sharding import PartitionSpec as P

BLK = 128
PARTS = 2
SKEW = 9.0
TILE = 256
MESH = pl.DeviceIdType.MESH


def gelu(x):
    return 0.5 * x * (1.0 + jnp.tanh(0.7978845608028654 * (x + 0.044715 * (x * x * x))))


def kernel(
    n, n_dp, capacity,
    routing, tasks, tokens, gate_weight, w_in_hbm, w_out_hbm, out,
    w_in, w_out, rings, cols, hidden, acc, pout, pin, xs, xr, gated, weights, rs_out, rs_in,
    w_sem, ag_s, ag_r, x_s, x_r, b_s, b_r, p_s, p_r, y_s, y_r, r_s, r_r,
):
    d_model = tokens.shape[1]
    chips = n_dp // 2
    half_ring = n // 2
    rows = BLK // PARTS
    mid = rows // 2
    wide = capacity * rows
    me = lax.axis_index("expert")
    my_dp = lax.axis_index("dp")
    my_x, my_core = my_dp // 2, my_dp % 2

    def pos_of(e):
        c, k = e % 2, e // 2
        return (1 - c) * k + c * (n - 1 - k)

    def expert_at(p):
        h = p // half_ring
        return (1 - h) * (2 * p) + h * (2 * (n - 1 - p) + 1)

    my_pos = pos_of(me)
    right = {"expert": expert_at((my_pos + 1) % n)}
    left = {"expert": expert_at((my_pos + n - 1) % n)}
    sibling = {"dp": my_x * 2 + 1 - my_core}

    def chip(k):
        return {"dp": ((my_x + k) % chips) * 2 + my_core}

    load_in = pltpu.make_async_copy(w_in_hbm.at[0], w_in, w_sem.at[0])
    load_out = pltpu.make_async_copy(w_out_hbm.at[0], w_out, w_sem.at[1])
    load_in.start()
    load_out.start()

    barrier = pltpu.get_barrier_semaphore()
    partners = [left, right, sibling] + [chip(k) for k in range(1, chips)]
    for partner in partners:
        pl.semaphore_signal(barrier, inc=1, device_id=partner, device_id_type=MESH)
    pl.semaphore_wait(barrier, len(partners))

    def remote(src, dst, send, recv, target):
        return pltpu.make_async_remote_copy(
            src_ref=src, dst_ref=dst, send_sem=send, recv_sem=recv,
            device_id=target, device_id_type=MESH,
        )

    sent = []

    def go(copy):
        copy.start()
        sent.append(copy)

    def span(s, way, last):
        if s != last:
            return pl.ds(0, rows)
        return pl.ds(0, mid) if way == 0 else pl.ds(mid, rows - mid)

    def ag_copy(h, way, s):
        source = (-s) % n if way == 0 else s % n
        target = (-s - 1) % n if way == 0 else (s + 1) % n
        part = span(s, way, half_ring - 1)
        if s == 0:
            begin = h * rows + (mid if way == 1 and half_ring == 1 else 0)
            src = tokens.at[pl.ds(begin, part.size)]
        else:
            src = rings[h].at[source, part]
        return remote(
            src, rings[h].at[target, part], ag_s.at[h, way, s], ag_r.at[h, way, s],
            right if way == 0 else left,
        )

    def ag_stage(h, s):
        for way in range(2):
            if s > 0:
                ag_copy(h, way, s - 1).wait_recv()
            go(ag_copy(h, way, s))

    taken, rank, count = [], [], 0
    for m in range(n):
        first, second = routing[m, 0], routing[m, 1]
        hit = jnp.where(first == me, 1, 0) + jnp.where(second == me, 1, 0)
        taken.append(hit)
        rank.append(count)
        count = count + hit
    slot_block, slot_other, slot_task, slot_valid = [], [], [], []
    for slot in range(capacity):
        at, other, task, valid = 0, 0, 0, 0
        for m in range(n):
            here = taken[m] * jnp.where(rank[m] == slot, 1, 0)
            at = at + here * ((pos_of(m) + n - my_pos) % n)
            other = other + here * (routing[m, 0] + routing[m, 1] - me)
            task = task + here * tasks[m]
            valid = valid + here
        slot_block.append(jnp.clip(at, 0, n - 1))
        slot_other.append(other)
        slot_task.append(task)
        slot_valid.append(valid)

    def slot_of(offset):
        e = expert_at((my_pos + offset + 2 * n) % n)
        hit = jnp.where(routing[e, 0] == me, 1, 0) + jnp.where(routing[e, 1] == me, 1, 0)
        before = 0
        for m in range(n):
            before = before + taken[m] * jnp.where(m < e, 1, 0)
        return jnp.clip(hit * before + (1 - hit) * capacity, 0, capacity)

    slots_at = [slot_of(k) for k in range(n)]

    def x_copy(h, k):
        return remote(
            cols.at[h, 0, 0], cols.at[h, chips - k, 0], x_s.at[h, k], x_r.at[h, chips - k], chip(k)
        )

    def b_copy(h, k):
        return remote(cols.at[h, k, 0], cols.at[h, k, 1], b_s.at[h, k], b_r.at[h, k], sibling)

    def select_stage(h):
        for way in range(2):
            ag_copy(h, way, half_ring - 1).wait_recv()
        rings[h][0] = tokens[h * rows : (h + 1) * rows, :]
        for slot in range(capacity):
            cols[h, 0, 0, slot * rows : (slot + 1) * rows, :] = rings[h][slot_block[slot]]
        mine = cols[h, 0, 0]
        logits = jnp.dot(mine, gate_weight[...], preferred_element_type=jnp.float32)
        column = lax.broadcasted_iota(jnp.int32, (rows, logits.shape[1]), 1)
        for slot in range(capacity):
            own = slot_task[slot] * n + me
            against = slot_task[slot] * n + slot_other[slot]
            sign = jnp.where(column == own, 1.0, 0.0) - jnp.where(column == against, 1.0, 0.0)
            gap = jnp.sum(
                logits[slot * rows : (slot + 1) * rows] * sign, axis=1, keepdims=True
            )
            gate = jax.nn.sigmoid(gap) * slot_valid[slot].astype(jnp.float32)
            weights[h, slot * rows : (slot + 1) * rows, :] = jnp.broadcast_to(gate, (rows, 128))
        for k in range(1, chips):
            go(x_copy(h, k))
        go(b_copy(h, 0))

    def x_recv(h, k):
        return remote(
            cols.at[h, 0, 0], cols.at[h, k, 0], x_s.at[h, chips - k], x_r.at[h, k], chip(chips - k)
        )

    def p_copy(h, k):
        return remote(pout.at[h, k], pin.at[h, k], p_s.at[h, k], p_r.at[h, k], sibling)

    def y_copy(h, k):
        return remote(
            xs.at[h, k], xr.at[h, chips - k], y_s.at[h, k], y_r.at[h, chips - k], chip(k)
        )

    def y_recv(h, k):
        return remote(
            xs.at[h, chips - k], xr.at[h, k], y_s.at[h, chips - k], y_r.at[h, k], chip(chips - k)
        )

    def forward_stage(h, k):
        x_recv(h, k).wait_recv()
        go(b_copy(h, k))

    def expert_stage(h, k):
        b_copy(h, k).wait_recv()
        lhs = cols.at[h, k]

        @pl.loop(0, w_in.shape[1] // TILE)
        def _(t):
            at = pl.ds(pl.multiple_of(t * TILE, TILE), TILE)
            x = lhs[...].reshape(2 * wide, d_model)
            y = jnp.dot(x, w_in[:, at], preferred_element_type=jnp.float32)
            hidden[:, at] = gelu(y).astype(jnp.bfloat16)

        @pl.loop(0, d_model // TILE)
        def _(t):
            at = pl.ds(pl.multiple_of(t * TILE, TILE), TILE)
            y = jnp.dot(hidden[...], w_out[:, at], preferred_element_type=jnp.float32)
            acc[h, k, :, at] = y[:wide]
            pout[h, k, :, at] = y[wide:].astype(jnp.bfloat16)

        go(p_copy(h, k))

    def return_stage(h, k):
        p_copy(h, k).wait_recv()
        xs[h, k] = (acc[h, k] + pin[h, k].astype(jnp.float32)).astype(jnp.bfloat16)
        go(y_copy(h, k))

    def gate_stage(h):
        p_copy(h, 0).wait_recv()
        for k in range(1, chips):
            y_recv(h, k).wait_recv()
        for slot in range(capacity):
            at = slice(slot * rows, (slot + 1) * rows)
            total = acc[h, 0, at, :] + pin[h, 0, at, :].astype(jnp.float32)
            for k in range(1, chips):
                total = total + xr[h, k, at, :].astype(jnp.float32)
            gated[h, slot] = (weights[h, at, :1] * total).astype(jnp.bfloat16)
        gated[h, capacity] = jnp.zeros((rows, d_model), jnp.bfloat16)

    def rs_copy(h, way, s):
        part = span(s, way, 0)
        return remote(
            rs_out.at[h, way, s, part], rs_in.at[h, way, s, part],
            r_s.at[h, way, s], r_r.at[h, way, s], right if way == 0 else left,
        )

    def share(h, offset):
        return gated[h, slots_at[offset % n]]

    def add(a, b):
        return (a.astype(jnp.float32) + b.astype(jnp.float32)).astype(jnp.bfloat16)

    def half(way):
        return slice(0, mid) if way == 0 else slice(mid, rows)

    def rs_stage(h, s):
        for way in range(2):
            offset = half_ring - s if way == 0 else s - half_ring
            rs_out[h, way, s] = share(h, offset)
            if s > 0:
                rs_copy(h, way, s - 1).wait_recv()
                at = half(way) if s == 1 else slice(0, rows)
                rs_out[h, way, s, at, :] = add(rs_out[h, way, s, at, :], rs_in[h, way, s - 1, at, :])
            go(rs_copy(h, way, s))

    def out_stage(h):
        for way in range(2):
            rs_copy(h, way, half_ring - 1).wait_recv()
        total = share(h, 0).astype(jnp.float32)
        for way in range(2):
            if half_ring > 1:
                total = total + rs_in[h, way, half_ring - 1].astype(jnp.float32)
        out[h * rows : (h + 1) * rows, :] = total.astype(jnp.bfloat16)

    def loaded(h):
        if h == 0:
            load_in.wait()
            load_out.wait()

    stages = []
    for h in range(PARTS):
        clock = h * SKEW

        def plan(when, *call):
            stages.append((when, len(stages), functools.partial(*call)))

        for s in range(half_ring):
            plan(h * 0.6 * SKEW + 4.0 * s, ag_stage, h, s)
        base = h * SKEW + 4.0 * half_ring
        plan(base, select_stage, h)
        plan(base + 1.0, loaded, h)
        plan(base + 1.1, expert_stage, h, 0)
        for k in range(1, chips):
            plan(base + 10.0 + k, forward_stage, h, k)
            plan(base + 12.0 + k, expert_stage, h, k)
            plan(base + 14.0 + k, return_stage, h, k)
        base = base + 24.0 + chips
        plan(base, gate_stage, h)
        for s in range(half_ring):
            plan(base + 0.5 + 4.0 * s, rs_stage, h, s)
        plan(base + 0.5 + 4.0 * half_ring, out_stage, h)
    for _, _, stage in sorted(stages, key=lambda item: item[:2]):
        stage()
    for copy in sent:
        copy.wait_send()


def shards(tokens, task_ids, routing, gate_weight, w_in, w_out):
    n = lax.axis_size("expert")
    n_dp = lax.axis_size("dp")
    d_model = tokens.shape[1]
    capacity = 2 * (tokens.shape[0] // BLK) + 1
    chips, half_ring = n_dp // 2, n // 2
    rows = BLK // PARTS
    wide = capacity * rows
    bf16 = jnp.bfloat16
    dma = pltpu.SemaphoreType.DMA
    vmem = pl.BlockSpec(memory_space=pltpu.VMEM)
    smem = pl.BlockSpec(memory_space=pltpu.SMEM)
    hbm = pl.BlockSpec(memory_space=pl.ANY)
    return pl.pallas_call(
        functools.partial(kernel, n, n_dp, capacity),
        out_shape=jax.ShapeDtypeStruct(tokens.shape, bf16),
        in_specs=[smem, smem, vmem, vmem, hbm, hbm],
        out_specs=vmem,
        scratch_shapes=[
            pltpu.VMEM(w_in.shape[1:], bf16),
            pltpu.VMEM(w_out.shape[1:], bf16),
            [pltpu.VMEM((n, rows, d_model), bf16) for _ in range(PARTS)],
            pltpu.VMEM((PARTS, chips, 2, wide, d_model), bf16),
            pltpu.VMEM((2 * wide, w_in.shape[2]), bf16),
            pltpu.VMEM((PARTS, chips, wide, d_model), jnp.float32),
            pltpu.VMEM((PARTS, chips, wide, d_model), bf16),
            pltpu.VMEM((PARTS, chips, wide, d_model), bf16),
            pltpu.VMEM((PARTS, chips, wide, d_model), bf16),
            pltpu.VMEM((PARTS, chips, wide, d_model), bf16),
            pltpu.VMEM((PARTS, capacity + 1, rows, d_model), bf16),
            pltpu.VMEM((PARTS, wide, 128), jnp.float32),
            pltpu.VMEM((PARTS, 2, half_ring, rows, d_model), bf16),
            pltpu.VMEM((PARTS, 2, half_ring, rows, d_model), bf16),
            dma((2,)),
            dma((PARTS, 2, half_ring)),
            dma((PARTS, 2, half_ring)),
            dma((PARTS, chips)),
            dma((PARTS, chips)),
            dma((PARTS, chips)),
            dma((PARTS, chips)),
            dma((PARTS, chips)),
            dma((PARTS, chips)),
            dma((PARTS, chips)),
            dma((PARTS, chips)),
            dma((PARTS, 2, half_ring)),
            dma((PARTS, 2, half_ring)),
        ],
        compiler_params=pltpu.CompilerParams(
            collective_id=0, has_side_effects=True, vmem_limit_bytes=64 * 1024 * 1024 - 65536
        ),
    )(routing, task_ids, tokens, gate_weight, w_in, w_out)


def solution(mesh):
    placed = (
        P(("dp", "expert"), None),
        P("dp"),
        P("dp", None),
        P(),
        P("expert", None, "dp"),
        P("expert", "dp", None),
    )
    return jax.shard_map(
        shards, mesh=mesh, in_specs=placed, out_specs=P(("dp", "expert"), None), check_vma=False
    )
```

```python
import functools

import jax
import jax.numpy as jnp
from jax import lax
from jax.experimental import pallas as pl
from jax.experimental.pallas import tpu as pltpu
from jax.sharding import PartitionSpec as P

BLK = 128
PARTS = 2
SKEW = 2.0
TILE = 256
MESH = pl.DeviceIdType.MESH


def gelu(x):
    return 0.5 * x * (1.0 + jnp.tanh(0.7978845608028654 * (x + 0.044715 * (x * x * x))))


def kernel(
    n, n_dp, capacity,
    routing, tasks, tokens, gate_weight, w_in_hbm, w_out_hbm, out,
    w_in, w_out, rings, cols, hidden, acc, pout, pin, xs, xr, gated, weights, rs_out, rs_in,
    w_sem, ag_s, ag_r, x_s, x_r, b_s, b_r, p_s, p_r, y_s, y_r, r_s, r_r,
):
    d_model = tokens.shape[1]
    chips = n_dp // 2
    half_ring = n // 2
    rows = BLK // PARTS
    mid = rows // 2
    wide = capacity * rows
    me = lax.axis_index("expert")
    my_dp = lax.axis_index("dp")
    my_x, my_core = my_dp // 2, my_dp % 2

    def pos_of(e):
        c, k = e % 2, e // 2
        return (1 - c) * k + c * (n - 1 - k)

    def expert_at(p):
        h = p // half_ring
        return (1 - h) * (2 * p) + h * (2 * (n - 1 - p) + 1)

    my_pos = pos_of(me)
    right = {"expert": expert_at((my_pos + 1) % n)}
    left = {"expert": expert_at((my_pos + n - 1) % n)}
    sibling = {"dp": my_x * 2 + 1 - my_core}

    def chip(k):
        return {"dp": ((my_x + k) % chips) * 2 + my_core}

    load_in = pltpu.make_async_copy(w_in_hbm.at[0], w_in, w_sem.at[0])
    load_out = pltpu.make_async_copy(w_out_hbm.at[0], w_out, w_sem.at[1])
    load_in.start()
    load_out.start()

    barrier = pltpu.get_barrier_semaphore()
    partners = [left, right, sibling] + [chip(k) for k in range(1, chips)]
    for partner in partners:
        pl.semaphore_signal(barrier, inc=1, device_id=partner, device_id_type=MESH)
    pl.semaphore_wait(barrier, len(partners))

    def remote(src, dst, send, recv, target):
        return pltpu.make_async_remote_copy(
            src_ref=src, dst_ref=dst, send_sem=send, recv_sem=recv,
            device_id=target, device_id_type=MESH,
        )

    sent = []

    def go(copy):
        copy.start()
        sent.append(copy)

    def span(s, way, last):
        if s != last:
            return pl.ds(0, rows)
        return pl.ds(0, mid) if way == 0 else pl.ds(mid, rows - mid)

    def ag_copy(h, way, s):
        source = (-s) % n if way == 0 else s % n
        target = (-s - 1) % n if way == 0 else (s + 1) % n
        part = span(s, way, half_ring - 1)
        if s == 0:
            begin = h * rows + (mid if way == 1 and half_ring == 1 else 0)
            src = tokens.at[pl.ds(begin, part.size)]
        else:
            src = rings[h].at[source, part]
        return remote(
            src, rings[h].at[target, part], ag_s.at[h, way, s], ag_r.at[h, way, s],
            right if way == 0 else left,
        )

    def ag_stage(h, s):
        for way in range(2):
            if s > 0:
                ag_copy(h, way, s - 1).wait_recv()
            go(ag_copy(h, way, s))

    for h in range(PARTS):
        ag_stage(h, 0)

    taken, rank, count = [], [], 0
    for m in range(n):
        first, second = routing[m, 0], routing[m, 1]
        hit = jnp.where(first == me, 1, 0) + jnp.where(second == me, 1, 0)
        taken.append(hit)
        rank.append(count)
        count = count + hit
    slot_block, slot_other, slot_task, slot_valid = [], [], [], []
    for slot in range(capacity):
        at, other, task, valid = 0, 0, 0, 0
        for m in range(n):
            here = taken[m] * jnp.where(rank[m] == slot, 1, 0)
            at = at + here * ((pos_of(m) + n - my_pos) % n)
            other = other + here * (routing[m, 0] + routing[m, 1] - me)
            task = task + here * tasks[m]
            valid = valid + here
        slot_block.append(jnp.clip(at, 0, n - 1))
        slot_other.append(other)
        slot_task.append(task)
        slot_valid.append(valid)

    def slot_of(offset):
        e = expert_at((my_pos + offset + 2 * n) % n)
        hit = jnp.where(routing[e, 0] == me, 1, 0) + jnp.where(routing[e, 1] == me, 1, 0)
        before = 0
        for m in range(n):
            before = before + taken[m] * jnp.where(m < e, 1, 0)
        return jnp.clip(hit * before + (1 - hit) * capacity, 0, capacity)

    slots_at = [slot_of(k) for k in range(n)]

    def x_copy(h, k):
        return remote(
            cols.at[h, 0, 0], cols.at[h, chips - k, 0], x_s.at[h, k], x_r.at[h, chips - k], chip(k)
        )

    def b_copy(h, k):
        return remote(cols.at[h, k, 0], cols.at[h, k, 1], b_s.at[h, k], b_r.at[h, k], sibling)

    def select_stage(h):
        for way in range(2):
            ag_copy(h, way, half_ring - 1).wait_recv()
        rings[h][0] = tokens[h * rows : (h + 1) * rows, :]
        for slot in range(capacity):
            cols[h, 0, 0, slot * rows : (slot + 1) * rows, :] = rings[h][slot_block[slot]]
        mine = cols[h, 0, 0]
        logits = jnp.dot(mine, gate_weight[...], preferred_element_type=jnp.float32)
        column = lax.broadcasted_iota(jnp.int32, (rows, logits.shape[1]), 1)
        for slot in range(capacity):
            own = slot_task[slot] * n + me
            against = slot_task[slot] * n + slot_other[slot]
            sign = jnp.where(column == own, 1.0, 0.0) - jnp.where(column == against, 1.0, 0.0)
            gap = jnp.sum(
                logits[slot * rows : (slot + 1) * rows] * sign, axis=1, keepdims=True
            )
            gate = jax.nn.sigmoid(gap) * slot_valid[slot].astype(jnp.float32)
            weights[h, slot * rows : (slot + 1) * rows, :] = jnp.broadcast_to(gate, (rows, 128))
        for k in range(1, chips):
            go(x_copy(h, k))
        go(b_copy(h, 0))

    def x_recv(h, k):
        return remote(
            cols.at[h, 0, 0], cols.at[h, k, 0], x_s.at[h, chips - k], x_r.at[h, k], chip(chips - k)
        )

    def p_copy(h, k):
        return remote(pout.at[h, k], pin.at[h, k], p_s.at[h, k], p_r.at[h, k], sibling)

    def y_copy(h, k):
        return remote(
            xs.at[h, k], xr.at[h, chips - k], y_s.at[h, k], y_r.at[h, chips - k], chip(k)
        )

    def y_recv(h, k):
        return remote(
            xs.at[h, chips - k], xr.at[h, k], y_s.at[h, chips - k], y_r.at[h, k], chip(chips - k)
        )

    def forward_stage(h, k):
        x_recv(h, k).wait_recv()
        go(b_copy(h, k))

    def expert_stage(h, k):
        b_copy(h, k).wait_recv()
        lhs = cols.at[h, k]

        @pl.loop(0, w_in.shape[1] // TILE)
        def _(t):
            at = pl.ds(pl.multiple_of(t * TILE, TILE), TILE)
            x = lhs[...].reshape(2 * wide, d_model)
            y = jnp.dot(x, w_in[:, at], preferred_element_type=jnp.float32)
            hidden[:, at] = gelu(y).astype(jnp.bfloat16)

        @pl.loop(0, d_model // TILE)
        def _(t):
            at = pl.ds(pl.multiple_of(t * TILE, TILE), TILE)
            y = jnp.dot(hidden[...], w_out[:, at], preferred_element_type=jnp.float32)
            acc[h, k, :, at] = y[:wide]
            pout[h, k, :, at] = y[wide:].astype(jnp.bfloat16)

        go(p_copy(h, k))

    def return_stage(h, k):
        p_copy(h, k).wait_recv()
        xs[h, k] = (acc[h, k] + pin[h, k].astype(jnp.float32)).astype(jnp.bfloat16)
        go(y_copy(h, k))

    def gate_stage(h):
        p_copy(h, 0).wait_recv()
        for k in range(1, chips):
            y_recv(h, k).wait_recv()
        for slot in range(capacity):
            at = slice(slot * rows, (slot + 1) * rows)
            total = acc[h, 0, at, :] + pin[h, 0, at, :].astype(jnp.float32)
            for k in range(1, chips):
                total = total + xr[h, k, at, :].astype(jnp.float32)
            gated[h, slot] = (weights[h, at, :1] * total).astype(jnp.bfloat16)
        gated[h, capacity] = jnp.zeros((rows, d_model), jnp.bfloat16)

    def rs_copy(h, way, s):
        part = span(s, way, 0)
        return remote(
            rs_out.at[h, way, s, part], rs_in.at[h, way, s, part],
            r_s.at[h, way, s], r_r.at[h, way, s], right if way == 0 else left,
        )

    def share(h, offset):
        return gated[h, slots_at[offset % n]]

    def add(a, b):
        return (a.astype(jnp.float32) + b.astype(jnp.float32)).astype(jnp.bfloat16)

    def half(way):
        return slice(0, mid) if way == 0 else slice(mid, rows)

    def rs_stage(h, s):
        for way in range(2):
            offset = half_ring - s if way == 0 else s - half_ring
            rs_out[h, way, s] = share(h, offset)
            if s > 0:
                rs_copy(h, way, s - 1).wait_recv()
                at = half(way) if s == 1 else slice(0, rows)
                rs_out[h, way, s, at, :] = add(rs_out[h, way, s, at, :], rs_in[h, way, s - 1, at, :])
            go(rs_copy(h, way, s))

    def out_stage(h):
        for way in range(2):
            rs_copy(h, way, half_ring - 1).wait_recv()
        total = share(h, 0).astype(jnp.float32)
        for way in range(2):
            if half_ring > 1:
                total = total + rs_in[h, way, half_ring - 1].astype(jnp.float32)
        out[h * rows : (h + 1) * rows, :] = total.astype(jnp.bfloat16)

    def loaded(h):
        if h == 0:
            load_in.wait()
            load_out.wait()

    stages = []
    for h in range(PARTS):

        def plan(when, *call):
            stages.append((when, len(stages), functools.partial(*call)))

        for s in range(1, half_ring):
            plan(h * 0.6 * SKEW + 4.0 * s, ag_stage, h, s)
        base = h * SKEW + 4.0 * half_ring
        plan(base, select_stage, h)
        plan(base + 1.0, loaded, h)
        plan(base + 1.1, expert_stage, h, 0)
        for k in range(1, chips):
            plan(base + 10.0 + k, forward_stage, h, k)
            plan(base + 12.0 + k, expert_stage, h, k)
            plan(base + 14.0 + k, return_stage, h, k)
        base = base + 24.0 + chips
        plan(base, gate_stage, h)
        for s in range(half_ring):
            plan(base + 0.5 + 4.0 * s, rs_stage, h, s)
        plan(base + 0.5 + 4.0 * half_ring, out_stage, h)
    for _, _, stage in sorted(stages, key=lambda item: item[:2]):
        stage()
    for copy in sent:
        copy.wait_send()


def shards(tokens, task_ids, routing, gate_weight, w_in, w_out):
    n = lax.axis_size("expert")
    n_dp = lax.axis_size("dp")
    d_model = tokens.shape[1]
    capacity = 2 * (tokens.shape[0] // BLK) + 1
    chips, half_ring = n_dp // 2, n // 2
    rows = BLK // PARTS
    wide = capacity * rows
    bf16 = jnp.bfloat16
    dma = pltpu.SemaphoreType.DMA
    vmem = pl.BlockSpec(memory_space=pltpu.VMEM)
    smem = pl.BlockSpec(memory_space=pltpu.SMEM)
    hbm = pl.BlockSpec(memory_space=pl.ANY)
    return pl.pallas_call(
        functools.partial(kernel, n, n_dp, capacity),
        out_shape=jax.ShapeDtypeStruct(tokens.shape, bf16),
        in_specs=[smem, smem, vmem, vmem, hbm, hbm],
        out_specs=vmem,
        scratch_shapes=[
            pltpu.VMEM(w_in.shape[1:], bf16),
            pltpu.VMEM(w_out.shape[1:], bf16),
            [pltpu.VMEM((n, rows, d_model), bf16) for _ in range(PARTS)],
            pltpu.VMEM((PARTS, chips, 2, wide, d_model), bf16),
            pltpu.VMEM((2 * wide, w_in.shape[2]), bf16),
            pltpu.VMEM((PARTS, chips, wide, d_model), jnp.float32),
            pltpu.VMEM((PARTS, chips, wide, d_model), bf16),
            pltpu.VMEM((PARTS, chips, wide, d_model), bf16),
            pltpu.VMEM((PARTS, chips, wide, d_model), bf16),
            pltpu.VMEM((PARTS, chips, wide, d_model), bf16),
            pltpu.VMEM((PARTS, capacity + 1, rows, d_model), bf16),
            pltpu.VMEM((PARTS, wide, 128), jnp.float32),
            pltpu.VMEM((PARTS, 2, half_ring, rows, d_model), bf16),
            pltpu.VMEM((PARTS, 2, half_ring, rows, d_model), bf16),
            dma((2,)),
            dma((PARTS, 2, half_ring)),
            dma((PARTS, 2, half_ring)),
            dma((PARTS, chips)),
            dma((PARTS, chips)),
            dma((PARTS, chips)),
            dma((PARTS, chips)),
            dma((PARTS, chips)),
            dma((PARTS, chips)),
            dma((PARTS, chips)),
            dma((PARTS, chips)),
            dma((PARTS, 2, half_ring)),
            dma((PARTS, 2, half_ring)),
        ],
        compiler_params=pltpu.CompilerParams(
            collective_id=0, has_side_effects=True, vmem_limit_bytes=64 * 1024 * 1024 - 65536
        ),
    )(routing, task_ids, tokens, gate_weight, w_in, w_out)


def solution(mesh):
    placed = (
        P(("dp", "expert"), None),
        P("dp"),
        P("dp", None),
        P(),
        P("expert", None, "dp"),
        P("expert", "dp", None),
    )
    return jax.shard_map(
        shards, mesh=mesh, in_specs=placed, out_specs=P(("dp", "expert"), None), check_vma=False
    )
```
